512 devices in a mesh: groups: 2 (over y), seq: 16 (over z), head: 8 (over x), rep: 2 (over core).
Axes of the slice: x: 8, y: 2, z: 16, core: 2. Of those that a mesh axis runs over, the one named last changes fastest.
The devices are a block of a 8x16x16 slice.
Arguments:
- kv_cache: bfloat16 [2, 1024, 8, 128, 256], P(None, ('groups', 'seq'), 'head', 'rep'), parts along dimension 1, may hold values from -6 to 6
- keep_list: int32 [4, 256], P('groups'), parts along dimension 0, may hold values from -1 to 511, as said below
- page_slot: int32 [4, 256], P('groups'), parts along dimension 0, may hold values from -1 to 255, as said below
Outputs:
- paged_cache: bfloat16 [2, 512, 8, 128, 256], P(None, ('groups', 'seq'), 'head', 'rep'), parts along dimension 1
- page_bounds: bfloat16 [2, 512, 8, 2, 128], P(None, ('groups', 'seq'), 'head'), parts along dimension 1
The draws below stay inside these ranges and needn't reach their ends.
There are 2 independent parts, one for each index of `groups`. The reference program is written for one: setup_inputs(seed, part) draws one part's arguments, and reference() takes and returns one part's arrays. A program takes and returns all parts, laid end to end along the dimension named above; each array names one. Nothing has to cross between parts.
Inputs may be any that keep to these rules, and one draw needn't show every extreme that they name: `keep_list`: row l holds count_l distinct block indices in rising order, then -1 in the remaining entries. Of one row, at most 16 listed blocks lie on one seq shard (blocks s * 32 to s * 32 + 31); row 0 reaches this on every shard. `page_slot`: entry (l, j) is the page of block keep_list[l, j]: distinct pages for the count_l listed blocks of a row, -1 after them. Of one row, at most 2 blocks of one seq shard go to pages of one owner (pages o * 16 to o * 16 + 15), and this is reached in every draw.
All inputs are finite; a program needn't handle non-finite values.
Results may differ from the reference program's by a relative error of at most 0.001.
Values may be sent and summed in bfloat16 or wider, within the bound.
No kernel may reach another device: no remote copies, remote signals or barrier semaphores. Data moves between devices by JAX's collectives and lax.ppermute only.
A program may use at most 64 MiB of HBM per device.

```python
import jax
import jax.numpy as jnp

KVH = 8
HD = 128
BLK = 128
LAYERS = 2
BLK_DEV = 32
BLOCKS = 512


def draw_plan(key):
    page_dev = BLK_DEV // 2
    seq_count = BLOCKS // BLK_DEV
    page_total = page_dev * seq_count
    keep_rows = []
    slot_rows = []
    for layer in range(LAYERS):
        layer_key = jax.random.fold_in(key, 7000 + layer)
        shift_key, local_key, used_key = jax.random.split(layer_key, 3)
        shuffled = jax.random.permutation(shift_key, seq_count).astype(jnp.int32)
        page_index = jnp.arange(page_dev, dtype=jnp.int32)
        shift_value = shuffled[jnp.maximum(page_index - 1, 0) % seq_count]
        owner_index = jnp.arange(seq_count, dtype=jnp.int32)
        source = (owner_index[:, None] + shift_value[None, :]) % seq_count
        scores = jax.random.randint(local_key, (seq_count, BLK_DEV), 0, 2 ** 20) * BLK_DEV + jnp.arange(BLK_DEV, dtype=jnp.int32)[None, :]
        local_order = jnp.argsort(scores, axis=1).astype(jnp.int32)
        local_block = local_order[source, jnp.broadcast_to(page_index[None, :], source.shape)]
        block_id = (source * BLK_DEV + local_block).reshape(-1).astype(jnp.int32)
        keep_count = page_total - layer * page_total // (2 * LAYERS)
        used = jax.random.permutation(used_key, page_total).astype(jnp.int32)[:keep_count]
        kept_blocks = block_id[used]
        sorter = jnp.argsort(kept_blocks)
        padding = jnp.full((page_total - keep_count,), -1, jnp.int32)
        keep_rows.append(jnp.concatenate([kept_blocks[sorter], padding]))
        slot_rows.append(jnp.concatenate([used[sorter], padding]))
    return (jnp.stack(keep_rows, axis=0).astype(jnp.int32), jnp.stack(slot_rows, axis=0).astype(jnp.int32))


def draw_keep_list(key, part):
    return draw_plan(key)[0]


def draw_page_slot(key, part):
    return draw_plan(key)[1]


def block_levels(rng, extent, pieces, least, largest):
    gain, own = 1.0, jax.random.fold_in(rng, 6)
    for position, parts in pieces:
        draws = jnp.exp(jax.random.uniform(jax.random.fold_in(own, position), (parts,), jnp.float32, least / len(pieces), largest / len(pieces)))
        gain = gain * jnp.repeat(draws, extent[position] // parts).reshape([-1 if axis == position else 1 for axis in range(len(extent))])
    return gain


def scatter_about(stream_key, dims, width, limit, cuts=(), held_as=jnp.bfloat16):
    factor_of = block_levels(stream_key, dims, cuts, -0.22, 0.18) if cuts else 1.0
    result = jax.random.normal(stream_key, dims, jnp.float32) * width * factor_of
    return jnp.minimum(jnp.maximum(result, -limit), limit).astype(held_as)


def setup_inputs(seed: int = 0, part: int = 0) -> dict:
    keys = jax.random.split(jax.random.key(seed), 4)
    part_splits = jax.random.split(jax.random.fold_in(keys[3], part), 4)
    kv_cache = scatter_about(part_splits[0], (LAYERS, BLOCKS, KVH, BLK, 2 * HD), 1.0, 6.0, ((1, 16), (2, 8), (3, 2)))
    keep_list = draw_keep_list(jax.random.fold_in(jax.random.fold_in(keys[3], part), 71), part)
    page_slot = draw_page_slot(jax.random.fold_in(jax.random.fold_in(keys[3], part), 71), part)
    return dict(kv_cache=kv_cache, keep_list=keep_list, page_slot=page_slot)


def reference(kv_cache, keep_list, page_slot):
    layer_count, page_count = keep_list.shape
    layer_pages = []
    for layer in range(layer_count):
        keep_count = page_count - (layer * page_count) // (2 * layer_count)
        kept_blocks = keep_list[layer, :keep_count].astype(jnp.int32)
        slot_list = page_slot[layer, :keep_count].astype(jnp.int32)
        chosen = kv_cache[layer][kept_blocks]
        empty_pages = jnp.zeros((page_count,) + kv_cache.shape[2:], kv_cache.dtype)
        layer_pages.append(empty_pages.at[slot_list].set(chosen))
    paged_cache = jnp.stack(layer_pages, axis=0)
    key_part = paged_cache[..., :HD]
    page_bounds = jnp.stack([jnp.max(key_part, axis=3), jnp.min(key_part, axis=3)], axis=3)
    return paged_cache, page_bounds
```

```python
import functools

import jax
import jax.numpy as jnp
from jax import lax
from jax.experimental import pallas as pl
from jax.experimental.pallas import tpu as pltpu
from jax.sharding import PartitionSpec as P


def copy_through(fetches, out_ref, stage, sem_in, sem_out):
    into = [
        pltpu.make_async_copy(source, stage.at[k], sem_in.at[k])
        for k, source in enumerate(fetches)
    ]
    back = [
        pltpu.make_async_copy(stage.at[k], out_ref.at[k], sem_out.at[k])
        for k in range(len(fetches))
    ]
    for copy in into:
        copy.start()
    for arrive, leave in zip(into, back):
        arrive.wait()
        leave.start()
    for copy in back:
        copy.wait()


def pack_kernel(index_ref, cache_ref, out_ref, stage, sem_in, sem_out):
    layers, owners = index_ref.shape
    fetches = [
        cache_ref.at[layer, index_ref[layer, owner], 0]
        for owner in range(owners)
        for layer in range(layers)
    ]
    copy_through(fetches, out_ref, stage, sem_in, sem_out)


def pick_kernel(index_ref, layer_ref, cache_ref, out_ref, stage, sem_in, sem_out):
    fetches = [cache_ref.at[layer_ref[k], index_ref[k], 0] for k in range(index_ref.shape[0])]
    copy_through(fetches, out_ref, stage, sem_in, sem_out)


def gather_blocks(kernel, scalars, cache, count):
    block = cache.shape[3:]
    return pl.pallas_call(
        kernel,
        grid_spec=pltpu.PrefetchScalarGridSpec(
            num_scalar_prefetch=len(scalars),
            grid=(1,),
            in_specs=[pl.BlockSpec(memory_space=pltpu.HBM)],
            out_specs=pl.BlockSpec(memory_space=pltpu.HBM),
            scratch_shapes=[
                pltpu.VMEM((count, *block), cache.dtype),
                pltpu.SemaphoreType.DMA((count,)),
                pltpu.SemaphoreType.DMA((count,)),
            ],
        ),
        out_shape=jax.ShapeDtypeStruct((count, *block), cache.dtype),
        compiler_params=pltpu.CompilerParams(vmem_limit_bytes=8 << 20),
    )(*scalars, cache)


def place_kernel(
    table_ref, many_ref, base_ref, left_ref, right_ref, extra_ref,
    out_ref, bounds_ref, empty, spare, rows, sem, spare_sem,
):
    pages, slots = out_ref.shape[0], base_ref.shape[0]
    head_width = base_ref.shape[-1] // 2
    empty[...] = jnp.zeros_like(empty)

    @pl.when(many_ref[0] != 0)
    def _():
        copy = pltpu.make_async_copy(extra_ref, spare, spare_sem)
        copy.start()
        copy.wait()

    def put(i, ref):
        pltpu.make_async_copy(ref, out_ref.at[i], sem.at[i]).start()
        keys = ref[:, :head_width].astype(jnp.float32)
        rows[pl.ds(2 * i, 1), :] = jnp.max(keys, axis=0, keepdims=True)
        rows[pl.ds(2 * i + 1, 1), :] = -jnp.min(keys, axis=0, keepdims=True)

    for i in range(pages):
        t = table_ref[i // table_ref.shape[1], i % table_ref.shape[1]]

        @pl.when(t < 0)
        def _():
            pltpu.make_async_copy(empty, out_ref.at[i], sem.at[i]).start()
            rows[pl.ds(2 * i, 2), :] = jnp.zeros((2, head_width), jnp.float32)

        @pl.when((t >= 0) & (t < slots))
        def _():
            put(i, base_ref.at[jnp.clip(t, 0, slots - 1)])

        @pl.when(t == slots)
        def _():
            put(i, left_ref)

        @pl.when(t == slots + 1)
        def _():
            put(i, right_ref)

        @pl.when(t >= slots + 2)
        def _():
            put(i, spare.at[jnp.clip(t - slots - 2, 0, slots - 1)])

    bounds_ref[...] = rows[...].astype(bounds_ref.dtype)
    for i in range(pages):
        pltpu.make_async_copy(empty, out_ref.at[i], sem.at[i]).wait()


def place_pages(table, many, base, left, right, extra, pages):
    block, head_width = base.shape[1:], base.shape[-1] // 2
    vmem = pl.BlockSpec(memory_space=pltpu.VMEM)
    hbm = pl.BlockSpec(memory_space=pltpu.HBM)
    return pl.pallas_call(
        place_kernel,
        grid_spec=pltpu.PrefetchScalarGridSpec(
            num_scalar_prefetch=2,
            grid=(1,),
            in_specs=[vmem, vmem, vmem, hbm],
            out_specs=[hbm, vmem],
            scratch_shapes=[
                pltpu.VMEM(block, base.dtype),
                pltpu.VMEM(base.shape, base.dtype),
                pltpu.VMEM((2 * pages, head_width), jnp.float32),
                pltpu.SemaphoreType.DMA((pages,)),
                pltpu.SemaphoreType.DMA,
            ],
        ),
        out_shape=[
            jax.ShapeDtypeStruct((pages, *block), base.dtype),
            jax.ShapeDtypeStruct((2 * pages, head_width), base.dtype),
        ],
        compiler_params=pltpu.CompilerParams(vmem_limit_bytes=8 << 20),
    )(table, many, base, left, right, extra)


def swap(block, shift, size):
    if shift == 0:
        return block
    return lax.ppermute(block, "seq", [(s, (s + shift) % size) for s in range(size)])


def on_device(kv_cache, keep_list, page_slot):
    layer_count, page_count = keep_list.shape
    blk_dev = kv_cache.shape[1]
    seq_count = lax.axis_size("seq")
    rep_count = lax.axis_size("rep")
    page_dev = page_count // seq_count
    slots = seq_count * layer_count
    me = lax.axis_index("seq")
    shards = jnp.arange(seq_count, dtype=jnp.int32)

    my_block = me * blk_dev
    my_page = shards * page_dev
    sent = (keep_list >= my_block) & (keep_list < my_block + blk_dev)
    owned = (page_slot[:, None, :] >= my_page[None, :, None]) & (
        page_slot[:, None, :] < my_page[None, :, None] + page_dev
    )
    local = jnp.where(sent, keep_list - my_block, -1)[:, None, :]
    first = jnp.min(jnp.where(owned & (local >= 0), local, blk_dev), axis=2)
    first = jnp.where(first == blk_dev, 0, first)
    payload = gather_blocks(pack_kernel, (first,), kv_cache, slots)

    def exchange(blocks):
        shaped = blocks.reshape(seq_count, layer_count, *blocks.shape[1:])
        moved = lax.all_to_all(shaped, "seq", split_axis=0, concat_axis=0, tiled=True)
        return moved.reshape(blocks.shape)

    base = exchange(payload)
    keep_list, page_slot, payload = lax.optimization_barrier((keep_list, page_slot, payload))

    def split(count):
        return count.bit_length() - 1

    source, owner = keep_list >> split(blk_dev), page_slot >> split(page_dev)
    local = jnp.where(source == me, keep_list - me * blk_dev, 0)[:, None, :]
    second = jnp.max(jnp.where(owner[:, None, :] == shards[None, :, None], local, 0), axis=2)
    position = jnp.arange(page_count, dtype=jnp.int32)
    pair = jnp.where(keep_list >= 0, source * seq_count + owner, -1 - position)
    again = jnp.any(
        (pair[:, :, None] == pair[:, None, :]) & (position[None, :] < position[:, None])[None], axis=2
    )
    shift = jnp.where(owner >= source, owner - source, owner - source + seq_count)
    active = jnp.any(again[:, None, :] & (shift[:, None, :] == shards[None, :, None]), axis=2)
    number = jnp.arange(slots, dtype=jnp.int32).reshape(layer_count, seq_count)
    none = jnp.int32(2 * slots)
    class_a = jnp.min(jnp.where(active, number, none))
    class_b = jnp.min(jnp.where(active & (number > class_a), number, none))
    many = jnp.any(active & (number > class_b)).astype(jnp.int32)
    shift_a = jnp.where(class_a < none, lax.rem(class_a, seq_count), 0)
    shift_b = jnp.where(class_b < none, lax.rem(class_b, seq_count), 0)
    flip = shift_a > shift_b
    class_a, class_b = jnp.where(flip, class_b, class_a), jnp.where(flip, class_a, class_b)
    shift_a, shift_b = jnp.where(flip, shift_b, shift_a), jnp.where(flip, shift_a, shift_b)
    classes = jnp.stack([class_a, class_b])
    shifts = jnp.stack([shift_a, shift_b])
    class_layer = jnp.where(classes < none, lax.div(classes, seq_count), 0)
    wanted = class_layer * seq_count + lax.rem(me + shifts, seq_count)
    wanted = wanted[:, None, None] == number[None]
    class_block = jnp.sum(jnp.where(wanted, second[None], 0), axis=(1, 2))
    pair_blocks = gather_blocks(pick_kernel, (class_block, class_layer), kv_cache, 2)

    page = me * page_dev + jnp.arange(page_dev, dtype=jnp.int32)
    held = jnp.max(
        jnp.where(page_slot[:, None, :] == page[None, :, None], keep_list[:, None, :], -1), axis=2
    )
    origin = held >> split(blk_dev)
    later = jnp.any(
        (origin[:, :, None] == origin[:, None, :]) & (held[:, None, :] < held[:, :, None]), axis=2
    )
    layers = jnp.arange(layer_count, dtype=jnp.int32)[:, None]
    slot = origin * layer_count + layers
    back = jnp.where(me >= origin, me - origin, me - origin + seq_count)
    moved_slot = jnp.where(layers * seq_count + back == class_a, slots, slots + 1)
    table = jnp.where(later, jnp.where(many > 0, slots + 2 + slot, moved_slot), slot)
    table = jnp.where(held < 0, -1, table).astype(jnp.int32)

    branches = [
        lambda one, two, one_by=a, two_by=b: (
            swap(one, one_by, seq_count),
            swap(two, two_by, seq_count),
        )
        for b in range(seq_count)
        for a in range(b + 1)
    ]
    branch = shift_b * (shift_b + 1) // 2 + shift_a
    branch, pair_blocks, table = lax.optimization_barrier((branch, pair_blocks, table))
    left, right = lax.switch(branch, branches, pair_blocks[0], pair_blocks[1])

    def all_seconds(state):
        rounds, index, _ = lax.optimization_barrier(state)
        return rounds - 1, index, exchange(gather_blocks(pack_kernel, (index,), kv_cache, slots))

    base, payload, many = lax.optimization_barrier((base, payload, many))
    _, _, extra = lax.while_loop(lambda state: state[0] > 0, all_seconds, (many, second, payload))

    pages, half = place_pages(
        table, many.reshape(1), base, left, right, extra, layer_count * page_dev
    )
    other = lax.ppermute(half, "rep", [(r, (r + 1) % rep_count) for r in range(rep_count)])
    width = half.shape[-1]
    high = jnp.maximum(half, other).reshape(layer_count, page_dev, 1, 2, width)
    is_low = lax.broadcasted_iota(jnp.int32, high.shape, 3) == 1
    page_bounds = jnp.where(is_low, -high, high)
    paged_cache = pages.reshape(layer_count, page_dev, *kv_cache.shape[2:])
    return paged_cache, page_bounds


def solution(mesh):
    in_specs = (
        P(None, ("groups", "seq"), "head", "rep", None),
        P("groups", None),
        P("groups", None),
    )
    out_specs = (
        P(None, ("groups", "seq"), "head", "rep", None),
        P(None, ("groups", "seq"), "head", None, None),
    )
    return jax.shard_map(
        on_device, mesh=mesh, in_specs=in_specs, out_specs=out_specs, check_vma=False
    )
```

```python
import functools

import jax
import jax.numpy as jnp
from jax import lax
from jax.experimental import pallas as pl
from jax.experimental.pallas import tpu as pltpu
from jax.sharding import PartitionSpec as P


def forward(fetches, leaves):
    for arrive, leave in zip(fetches, leaves):
        arrive.wait()
        leave.start()
    for leave in leaves:
        leave.wait()


def pack_kernel(index_ref, cache_ref, out_ref, stage, sem_in, sem_out):
    layers, owners = index_ref.shape
    keys = [(layer, owner) for owner in range(owners) for layer in range(layers)]
    fetches = [
        pltpu.make_async_copy(
            cache_ref.at[layer, index_ref[layer, owner], 0], stage.at[k], sem_in.at[k]
        )
        for k, (layer, owner) in enumerate(keys)
    ]
    leaves = [
        pltpu.make_async_copy(stage.at[k], out_ref.at[k], sem_out.at[k]) for k in range(len(keys))
    ]
    for copy in fetches:
        copy.start()
    forward(fetches, leaves)


def pack_seconds(index, cache, count):
    block = cache.shape[3:]
    return pl.pallas_call(
        pack_kernel,
        grid_spec=pltpu.PrefetchScalarGridSpec(
            num_scalar_prefetch=1,
            grid=(1,),
            in_specs=[pl.BlockSpec(memory_space=pltpu.HBM)],
            out_specs=pl.BlockSpec(memory_space=pltpu.HBM),
            scratch_shapes=[
                pltpu.VMEM((count, *block), cache.dtype),
                pltpu.SemaphoreType.DMA((count,)),
                pltpu.SemaphoreType.DMA((count,)),
            ],
        ),
        out_shape=jax.ShapeDtypeStruct((count, *block), cache.dtype),
        compiler_params=pltpu.CompilerParams(vmem_limit_bytes=8 << 20),
    )(index, cache)


def plan_kernel(
    owners, blk_dev, page_dev,
    keep_ref, slot_ref, cache_ref,
    payload_ref, left_ref, right_ref, table_ref, second_ref, choice_ref,
    stage, lists, held_lists, sem_in, sem_out, sem_list,
):
    layers, entries = keep_ref.shape
    slots, none = owners * layers, 2 * owners * layers
    late = 8 * slots
    me = lax.axis_index("seq")
    block_bits, page_bits = blk_dev.bit_length() - 1, page_dev.bit_length() - 1

    row = lax.broadcasted_iota(jnp.int32, (owners, entries), 0)
    square_row = lax.broadcasted_iota(jnp.int32, (owners, owners), 0)
    square_lane = lax.broadcasted_iota(jnp.int32, (owners, owners), 1)
    lane = lax.broadcasted_iota(jnp.int32, (owners, lists.shape[1]), 1)

    def most(values):
        return jnp.max(values.astype(jnp.float32), axis=1, keepdims=True).astype(jnp.int32)

    tables = jnp.zeros(lists.shape, jnp.int32)
    for layer in range(layers):
        keep, slot = keep_ref[pl.ds(layer, 1), :], slot_ref[pl.ds(layer, 1), :]
        source, owner = keep >> block_bits, slot >> page_bits
        chosen = (owner == row) & (source == me)
        local = keep - me * blk_dev
        first = blk_dev - 1 - most(jnp.where(chosen, blk_dev - 1 - local, 0))
        second = most(jnp.where(chosen, local, 0))
        gap = owner - source
        gap = jnp.where(gap < 0, gap + owners, gap)
        by_gap = jnp.where((gap == row) & (keep >= 0), 1.0, 0.0).astype(jnp.bfloat16)
        by_source = jnp.where(source == row, 1.0, 0.0).astype(jnp.bfloat16)
        count = lax.dot_general(
            by_gap, by_source, (((1,), (1,)), ((), ())), preferred_element_type=jnp.float32
        )
        active = (jnp.max(count, axis=1, keepdims=True) > 1.5).astype(jnp.int32)
        held = most(jnp.where(slot == me * page_dev + row, keep, -1))
        across = jnp.max(
            jnp.where(square_row == square_lane, held, -1).astype(jnp.float32), axis=0, keepdims=True
        ).astype(jnp.int32)
        origin = held >> block_bits
        again = most(jnp.where((across >> block_bits == origin) & (across < held), 1, 0))
        found = jnp.where(held < 0, -1, origin * layers + layer + again * late)
        for kind, values in enumerate((first, second, active, found)):
            tables = jnp.where(lane == kind * layers + layer, values, tables)
    lists[...] = tables
    copy = pltpu.make_async_copy(lists, held_lists, sem_list)
    copy.start()
    copy.wait()

    def listed(kind, layer, index):
        return held_lists[index, kind * layers + layer]

    def fetch(layer, index, k):
        return pltpu.make_async_copy(cache_ref.at[layer, index, 0], stage.at[k], sem_in.at[k])

    fetches = []
    for owner in range(owners):
        for layer in range(layers):
            fetches.append(fetch(layer, listed(0, layer, owner), len(fetches)))
            fetches[-1].start()

    class_a, class_b, total = jnp.int32(none), jnp.int32(none), jnp.int32(0)
    for layer in range(layers):
        for gap in range(owners):
            on = listed(2, layer, gap)
            class_b = jnp.where((on > 0) & (total == 1), layer * owners + gap, class_b)
            class_a = jnp.where((on > 0) & (total == 0), layer * owners + gap, class_a)
            total = total + on
    many = (total > 2).astype(jnp.int32)
    shift_a = jnp.where(class_a < none, lax.rem(class_a, owners), 0)
    shift_b = jnp.where(class_b < none, lax.rem(class_b, owners), 0)
    flip = shift_a > shift_b
    class_a, class_b = jnp.where(flip, class_b, class_a), jnp.where(flip, class_a, class_b)
    shift_a, shift_b = jnp.where(flip, shift_b, shift_a), jnp.where(flip, shift_a, shift_b)
    for number, by in ((class_a, shift_a), (class_b, shift_b)):
        layer = jnp.where(number < none, lax.div(number, owners), 0)
        index = listed(1, layer, lax.rem(me + by, owners))
        fetches.append(fetch(layer, index, len(fetches)))
        fetches[-1].start()
    choice_ref[0] = lax.div(shift_b * (shift_b + 1), 2) + shift_a
    choice_ref[1] = many

    for layer in range(layers):
        for index in range(owners):
            second_ref[layer, index] = listed(1, layer, index)
            slot = listed(3, layer, index)
            plain = jnp.where(slot >= late, slot - late, slot)
            back = lax.rem(me - lax.div(plain, layers) + owners, owners)
            moved = jnp.where(layer * owners + back == class_a, slots, slots + 1)
            moved = jnp.where(many > 0, slots + 2 + plain, moved)
            table_ref[layer, index] = jnp.where(slot >= late, moved, slot)

    targets = [payload_ref.at[k] for k in range(slots)] + [left_ref, right_ref]
    leaves = [
        pltpu.make_async_copy(stage.at[k], target, sem_out.at[k])
        for k, target in enumerate(targets)
    ]
    forward(fetches, leaves)


def plan_and_pack(keep_list, page_slot, cache, owners):
    layers, entries = keep_list.shape
    slots, block = owners * layers, cache.shape[3:]
    page_dev = entries // owners
    vmem = pl.BlockSpec(memory_space=pltpu.VMEM)
    smem = pl.BlockSpec(memory_space=pltpu.SMEM)
    hbm = pl.BlockSpec(memory_space=pltpu.HBM)
    one = jax.ShapeDtypeStruct(block, cache.dtype)
    return pl.pallas_call(
        functools.partial(plan_kernel, owners, cache.shape[1], page_dev),
        in_specs=[vmem, vmem, hbm],
        out_specs=[hbm, hbm, hbm, smem, smem, smem],
        scratch_shapes=[
            pltpu.VMEM((slots + 2, *block), cache.dtype),
            pltpu.VMEM((owners, 128), jnp.int32),
            pltpu.SMEM((owners, 128), jnp.int32),
            pltpu.SemaphoreType.DMA((slots + 2,)),
            pltpu.SemaphoreType.DMA((slots + 2,)),
            pltpu.SemaphoreType.DMA,
        ],
        out_shape=[
            jax.ShapeDtypeStruct((slots, *block), cache.dtype),
            one,
            one,
            jax.ShapeDtypeStruct((layers, page_dev), jnp.int32),
            jax.ShapeDtypeStruct((layers, owners), jnp.int32),
            jax.ShapeDtypeStruct((2,), jnp.int32),
        ],
        compiler_params=pltpu.CompilerParams(vmem_limit_bytes=8 << 20),
    )(keep_list, page_slot, cache)


def place_kernel(
    table_ref, many_ref, base_ref, left_ref, right_ref, extra_ref,
    out_ref, bounds_ref, empty, spare, rows, sem, spare_sem,
):
    pages, slots = out_ref.shape[0], base_ref.shape[0]
    head_width = base_ref.shape[-1] // 2
    empty[...] = jnp.zeros_like(empty)

    @pl.when(many_ref[0] != 0)
    def _():
        copy = pltpu.make_async_copy(extra_ref, spare, spare_sem)
        copy.start()
        copy.wait()

    def put(i, ref):
        pltpu.make_async_copy(ref, out_ref.at[i], sem.at[i]).start()
        keys = ref[:, :head_width].astype(jnp.float32)
        rows[pl.ds(2 * i, 1), :] = jnp.max(keys, axis=0, keepdims=True)
        rows[pl.ds(2 * i + 1, 1), :] = -jnp.min(keys, axis=0, keepdims=True)

    for i in range(pages):
        t = table_ref[i // table_ref.shape[1], i % table_ref.shape[1]]

        @pl.when(t < 0)
        def _():
            pltpu.make_async_copy(empty, out_ref.at[i], sem.at[i]).start()
            rows[pl.ds(2 * i, 2), :] = jnp.zeros((2, head_width), jnp.float32)

        @pl.when((t >= 0) & (t < slots))
        def _():
            put(i, base_ref.at[jnp.clip(t, 0, slots - 1)])

        @pl.when(t == slots)
        def _():
            put(i, left_ref)

        @pl.when(t == slots + 1)
        def _():
            put(i, right_ref)

        @pl.when(t >= slots + 2)
        def _():
            put(i, spare.at[jnp.clip(t - slots - 2, 0, slots - 1)])

    bounds_ref[...] = rows[...].astype(bounds_ref.dtype)
    for i in range(pages):
        pltpu.make_async_copy(empty, out_ref.at[i], sem.at[i]).wait()


def place_pages(table, many, base, left, right, extra, pages):
    block, head_width = base.shape[1:], base.shape[-1] // 2
    vmem = pl.BlockSpec(memory_space=pltpu.VMEM)
    hbm = pl.BlockSpec(memory_space=pltpu.HBM)
    return pl.pallas_call(
        place_kernel,
        grid_spec=pltpu.PrefetchScalarGridSpec(
            num_scalar_prefetch=2,
            grid=(1,),
            in_specs=[vmem, vmem, vmem, hbm],
            out_specs=[hbm, vmem],
            scratch_shapes=[
                pltpu.VMEM(block, base.dtype),
                pltpu.VMEM(base.shape, base.dtype),
                pltpu.VMEM((2 * pages, head_width), jnp.float32),
                pltpu.SemaphoreType.DMA((pages,)),
                pltpu.SemaphoreType.DMA,
            ],
        ),
        out_shape=[
            jax.ShapeDtypeStruct((pages, *block), base.dtype),
            jax.ShapeDtypeStruct((2 * pages, head_width), base.dtype),
        ],
        compiler_params=pltpu.CompilerParams(vmem_limit_bytes=8 << 20),
    )(table, many, base, left, right, extra)


def swap(block, shift, size):
    if shift == 0:
        return block
    return lax.ppermute(block, "seq", [(s, (s + shift) % size) for s in range(size)])


def on_device(kv_cache, keep_list, page_slot):
    layer_count, page_count = keep_list.shape
    seq_count = lax.axis_size("seq")
    page_dev = page_count // seq_count
    slots = seq_count * layer_count

    def exchange(blocks):
        shaped = blocks.reshape(seq_count, layer_count, *blocks.shape[1:])
        moved = lax.all_to_all(shaped, "seq", split_axis=0, concat_axis=0, tiled=True)
        return moved.reshape(blocks.shape)

    payload, one, two, table, second, choice = plan_and_pack(
        keep_list, page_slot, kv_cache, seq_count
    )
    branch, many = choice[0], choice[1]
    base = exchange(payload)

    branches = [
        lambda one, two, one_by=a, two_by=b: (
            swap(one, one_by, seq_count),
            swap(two, two_by, seq_count),
        )
        for b in range(seq_count)
        for a in range(b + 1)
    ]
    left, right = lax.switch(branch, branches, one, two)

    def all_seconds(state):
        rounds, index, _ = lax.optimization_barrier(state)
        return rounds - 1, index, exchange(pack_seconds(index, kv_cache, slots))

    base, payload, many = lax.optimization_barrier((base, payload, many))
    _, _, extra = lax.while_loop(lambda state: state[0] > 0, all_seconds, (many, second, payload))

    pages, half = place_pages(
        table, many.reshape(1), base, left, right, extra, layer_count * page_dev
    )
    halves = lax.all_gather(half, "rep")
    high = jnp.max(halves, axis=0).reshape(layer_count, page_dev, 1, 2, half.shape[-1])
    is_low = lax.broadcasted_iota(jnp.int32, high.shape, 3) == 1
    page_bounds = jnp.where(is_low, 0 - high, high)
    paged_cache = pages.reshape(layer_count, page_dev, *kv_cache.shape[2:])
    return paged_cache, page_bounds


def solution(mesh):
    in_specs = (
        P(None, ("groups", "seq"), "head", "rep", None),
        P("groups", None),
        P("groups", None),
    )
    out_specs = (
        P(None, ("groups", "seq"), "head", "rep", None),
        P(None, ("groups", "seq"), "head", None, None),
    )
    return jax.shard_map(
        on_device, mesh=mesh, in_specs=in_specs, out_specs=out_specs, check_vma=False
    )
```

```python
import functools

import jax
import jax.numpy as jnp
from jax import lax
from jax.experimental import pallas as pl
from jax.experimental.pallas import tpu as pltpu
from jax.sharding import PartitionSpec as P


def forward(fetches, leaves):
    for arrive, leave in zip(fetches, leaves):
        arrive.wait()
        leave.start()
    for leave in leaves:
        leave.wait()


def pack_kernel(index_ref, cache_ref, out_ref, stage, sem_in, sem_out):
    layers, owners = index_ref.shape
    keys = [(layer, owner) for owner in range(owners) for layer in range(layers)]
    fetches = [
        pltpu.make_async_copy(
            cache_ref.at[layer, index_ref[layer, owner], 0], stage.at[k], sem_in.at[k]
        )
        for k, (layer, owner) in enumerate(keys)
    ]
    leaves = [
        pltpu.make_async_copy(stage.at[k], out_ref.at[k], sem_out.at[k]) for k in range(len(keys))
    ]
    for copy in fetches:
        copy.start()
    forward(fetches, leaves)


def pack_seconds(index, cache, count):
    block = cache.shape[3:]
    return pl.pallas_call(
        pack_kernel,
        grid_spec=pltpu.PrefetchScalarGridSpec(
            num_scalar_prefetch=1,
            grid=(1,),
            in_specs=[pl.BlockSpec(memory_space=pltpu.HBM)],
            out_specs=pl.BlockSpec(memory_space=pltpu.HBM),
            scratch_shapes=[
                pltpu.VMEM((count, *block), cache.dtype),
                pltpu.SemaphoreType.DMA((count,)),
                pltpu.SemaphoreType.DMA((count,)),
            ],
        ),
        out_shape=jax.ShapeDtypeStruct((count, *block), cache.dtype),
        compiler_params=pltpu.CompilerParams(vmem_limit_bytes=8 << 20),
    )(index, cache)


def plan_kernel(
    owners, blk_dev, page_dev,
    keep_hbm, slot_hbm, cache_ref,
    payload_ref, left_ref, right_ref, table_ref, second_ref, branch_ref, many_ref,
    keep_ref, slot_ref, stage, lists, held_lists, sem_in, sem_out, sem_list,
):
    inputs = [
        pltpu.make_async_copy(keep_hbm, keep_ref, sem_in.at[0]),
        pltpu.make_async_copy(slot_hbm, slot_ref, sem_in.at[1]),
    ]
    for copy in inputs:
        copy.start()
    layers, entries = keep_ref.shape
    slots, none = owners * layers, 2 * owners * layers
    late = 8 * slots
    me = lax.axis_index("seq")
    block_bits, page_bits = blk_dev.bit_length() - 1, page_dev.bit_length() - 1

    row = lax.broadcasted_iota(jnp.int32, (owners, entries), 0)
    square_row = lax.broadcasted_iota(jnp.int32, (owners, owners), 0)
    square_lane = lax.broadcasted_iota(jnp.int32, (owners, owners), 1)
    lane = lax.broadcasted_iota(jnp.int32, (owners, lists.shape[1]), 1)

    def most(values):
        return jnp.max(values.astype(jnp.float32), axis=1, keepdims=True).astype(jnp.int32)

    for copy in inputs:
        copy.wait()
    tables = jnp.zeros(lists.shape, jnp.int32)
    for layer in range(layers):
        keep, slot = keep_ref[pl.ds(layer, 1), :], slot_ref[pl.ds(layer, 1), :]
        source, owner = keep >> block_bits, slot >> page_bits
        chosen = (owner == row) & (source == me)
        local = keep - me * blk_dev
        first = blk_dev - 1 - most(jnp.where(chosen, blk_dev - 1 - local, 0))
        second = most(jnp.where(chosen, local, 0))
        gap = owner - source
        gap = jnp.where(gap < 0, gap + owners, gap)
        by_gap = jnp.where((gap == row) & (keep >= 0), 1.0, 0.0).astype(jnp.bfloat16)
        by_source = jnp.where(source == row, 1.0, 0.0).astype(jnp.bfloat16)
        count = lax.dot_general(
            by_gap, by_source, (((1,), (1,)), ((), ())), preferred_element_type=jnp.float32
        )
        active = (jnp.max(count, axis=1, keepdims=True) > 1.5).astype(jnp.int32)
        held = most(jnp.where(slot == me * page_dev + row, keep, -1))
        across = jnp.max(
            jnp.where(square_row == square_lane, held, -1).astype(jnp.float32), axis=0, keepdims=True
        ).astype(jnp.int32)
        origin = held >> block_bits
        again = most(jnp.where((across >> block_bits == origin) & (across < held), 1, 0))
        found = jnp.where(held < 0, -1, origin * layers + layer + again * late)
        for kind, values in enumerate((first, second, active, found)):
            tables = jnp.where(lane == kind * layers + layer, values, tables)
    lists[...] = tables
    copy = pltpu.make_async_copy(lists, held_lists, sem_list)
    copy.start()
    copy.wait()

    def listed(kind, layer, index):
        return held_lists[index, kind * layers + layer]

    def fetch(layer, index, k):
        return pltpu.make_async_copy(cache_ref.at[layer, index, 0], stage.at[k], sem_in.at[k])

    fetches = []
    for owner in range(owners):
        for layer in range(layers):
            fetches.append(fetch(layer, listed(0, layer, owner), len(fetches)))
            fetches[-1].start()

    class_a, class_b, total = jnp.int32(none), jnp.int32(none), jnp.int32(0)
    for layer in range(layers):
        for gap in range(owners):
            on = listed(2, layer, gap)
            class_b = jnp.where((on > 0) & (total == 1), layer * owners + gap, class_b)
            class_a = jnp.where((on > 0) & (total == 0), layer * owners + gap, class_a)
            total = total + on
    many = (total > 2).astype(jnp.int32)
    shift_a = jnp.where(class_a < none, lax.rem(class_a, owners), 0)
    shift_b = jnp.where(class_b < none, lax.rem(class_b, owners), 0)
    flip = shift_a > shift_b
    class_a, class_b = jnp.where(flip, class_b, class_a), jnp.where(flip, class_a, class_b)
    shift_a, shift_b = jnp.where(flip, shift_b, shift_a), jnp.where(flip, shift_a, shift_b)
    for number, by in ((class_a, shift_a), (class_b, shift_b)):
        layer = jnp.where(number < none, lax.div(number, owners), 0)
        index = listed(1, layer, lax.rem(me + by, owners))
        fetches.append(fetch(layer, index, len(fetches)))
        fetches[-1].start()
    branch_ref[0] = lax.div(shift_b * (shift_b + 1), 2) + shift_a
    many_ref[0] = many

    for layer in range(layers):
        for index in range(owners):
            second_ref[layer, index] = listed(1, layer, index)
            slot = listed(3, layer, index)
            plain = jnp.where(slot >= late, slot - late, slot)
            back = lax.rem(me - lax.div(plain, layers) + owners, owners)
            moved = jnp.where(layer * owners + back == class_a, slots, slots + 1)
            moved = jnp.where(many > 0, slots + 3 + plain, moved)
            moved = jnp.where(slot >= late, moved, slot)
            table_ref[layer, index] = jnp.where(slot < 0, slots + 2, moved)

    targets = [payload_ref.at[k] for k in range(slots)] + [left_ref, right_ref]
    leaves = [
        pltpu.make_async_copy(stage.at[k], target, sem_out.at[k])
        for k, target in enumerate(targets)
    ]
    forward(fetches, leaves)


def plan_and_pack(keep_list, page_slot, cache, owners):
    layers, entries = keep_list.shape
    slots, block = owners * layers, cache.shape[3:]
    page_dev = entries // owners
    smem = pl.BlockSpec(memory_space=pltpu.SMEM)
    hbm = pl.BlockSpec(memory_space=pltpu.HBM)
    one = jax.ShapeDtypeStruct(block, cache.dtype)
    return pl.pallas_call(
        functools.partial(plan_kernel, owners, cache.shape[1], page_dev),
        in_specs=[hbm, hbm, hbm],
        out_specs=[hbm, hbm, hbm, smem, smem, smem, smem],
        scratch_shapes=[
            pltpu.VMEM(keep_list.shape, jnp.int32),
            pltpu.VMEM(page_slot.shape, jnp.int32),
            pltpu.VMEM((slots + 2, *block), cache.dtype),
            pltpu.VMEM((owners, 128), jnp.int32),
            pltpu.SMEM((owners, 128), jnp.int32),
            pltpu.SemaphoreType.DMA((slots + 2,)),
            pltpu.SemaphoreType.DMA((slots + 2,)),
            pltpu.SemaphoreType.DMA,
        ],
        out_shape=[
            jax.ShapeDtypeStruct((slots, *block), cache.dtype),
            one,
            one,
            jax.ShapeDtypeStruct((layers, page_dev), jnp.int32),
            jax.ShapeDtypeStruct((layers, owners), jnp.int32),
            jax.ShapeDtypeStruct((1,), jnp.int32),
            jax.ShapeDtypeStruct((1,), jnp.int32),
        ],
        compiler_params=pltpu.CompilerParams(vmem_limit_bytes=60 << 20),
    )(keep_list, page_slot, cache)


def place_kernel(
    table_ref, many_ref, base_ref, left_ref, right_ref, extra_ref,
    out_ref, bounds_ref, spare, high, low, rows, sem, spare_sem,
):
    layers, page_dev = table_ref.shape
    slots, head_width = base_ref.shape[0], base_ref.shape[-1] // 2
    pages = layers * page_dev
    spare[0] = left_ref[...]
    spare[1] = right_ref[...]
    spare[2] = jnp.zeros_like(left_ref)

    def entry(i):
        return table_ref[i // page_dev, i % page_dev]

    for i in range(pages):
        t = entry(i)

        @pl.when(t < slots)
        def _():
            block = base_ref.at[jnp.minimum(t, slots - 1)]
            pltpu.make_async_copy(block, out_ref.at[i], sem).start()

    def extremes(k, ref):
        keys = ref[:, :head_width]
        high[pl.ds(k, 1), :] = jnp.max(keys, axis=0, keepdims=True).astype(jnp.float32)
        low[pl.ds(k, 1), :] = -jnp.min(keys, axis=0, keepdims=True).astype(jnp.float32)

    for k in range(slots):
        extremes(k, base_ref.at[k])
    for k in range(3):
        extremes(slots + k, spare.at[k])

    @pl.when(many_ref[0] != 0)
    def _():
        copy = pltpu.make_async_copy(extra_ref, spare.at[pl.ds(3, slots)], spare_sem)
        copy.start()
        copy.wait()

        @pl.loop(0, slots)
        def _(k):
            extremes(slots + 3 + k, spare.at[3 + k])

    for i in range(pages):
        t = entry(i)

        @pl.when(t >= slots)
        def _():
            block = spare.at[jnp.maximum(t - slots, 0)]
            pltpu.make_async_copy(block, out_ref.at[i], sem).start()

        rows[pl.ds(2 * i, 1), :] = high[pl.ds(t, 1), :]
        rows[pl.ds(2 * i + 1, 1), :] = low[pl.ds(t, 1), :]

    bounds_ref[...] = rows[...].astype(bounds_ref.dtype)
    pltpu.make_async_copy(out_ref, out_ref, sem).wait()


def place_pages(table, many, base, left, right, extra, pages):
    block, head_width = base.shape[1:], base.shape[-1] // 2
    vmem = pl.BlockSpec(memory_space=pltpu.VMEM)
    hbm = pl.BlockSpec(memory_space=pltpu.HBM)
    return pl.pallas_call(
        place_kernel,
        grid_spec=pltpu.PrefetchScalarGridSpec(
            num_scalar_prefetch=2,
            grid=(1,),
            in_specs=[vmem, vmem, vmem, hbm],
            out_specs=[hbm, vmem],
            scratch_shapes=[
                pltpu.VMEM((3 + base.shape[0], *block), base.dtype),
                pltpu.VMEM((3 + 2 * base.shape[0], head_width), jnp.float32),
                pltpu.VMEM((3 + 2 * base.shape[0], head_width), jnp.float32),
                pltpu.VMEM((2 * pages, head_width), jnp.float32),
                pltpu.SemaphoreType.DMA,
                pltpu.SemaphoreType.DMA,
            ],
        ),
        out_shape=[
            jax.ShapeDtypeStruct((pages, *block), base.dtype),
            jax.ShapeDtypeStruct((2 * pages, head_width), base.dtype),
        ],
        compiler_params=pltpu.CompilerParams(vmem_limit_bytes=8 << 20),
    )(table, many, base, left, right, extra)


def swap(block, shift, size):
    if shift == 0:
        return block
    return lax.ppermute(block, "seq", [(s, (s + shift) % size) for s in range(size)])


def on_device(kv_cache, keep_list, page_slot):
    layer_count, page_count = keep_list.shape
    seq_count = lax.axis_size("seq")
    page_dev = page_count // seq_count
    slots = seq_count * layer_count

    def exchange(blocks):
        shaped = blocks.reshape(seq_count, layer_count, *blocks.shape[1:])
        moved = lax.all_to_all(shaped, "seq", split_axis=0, concat_axis=0, tiled=True)
        return moved.reshape(blocks.shape)

    payload, one, two, table, second, branch, many = plan_and_pack(
        keep_list, page_slot, kv_cache, seq_count
    )
    branch, many = branch.reshape(()), many.reshape(())
    base = exchange(payload)

    branches = [
        lambda one, two, one_by=a, two_by=b: (
            swap(one, one_by, seq_count),
            swap(two, two_by, seq_count),
        )
        for b in range(seq_count)
        for a in range(b + 1)
    ]
    left, right = lax.switch(branch, branches, one, two)

    def all_seconds(state):
        rounds, index, _ = lax.optimization_barrier(state)
        return rounds - 1, index, exchange(pack_seconds(index, kv_cache, slots))

    base, payload, many = lax.optimization_barrier((base, payload, many))
    _, _, extra = lax.while_loop(lambda state: state[0] > 0, all_seconds, (many, second, payload))

    pages, half = place_pages(
        table, many.reshape(1), base, left, right, extra, layer_count * page_dev
    )
    halves = lax.all_gather(half, "rep")
    high = jnp.max(halves, axis=0).reshape(layer_count, page_dev, 1, 2, half.shape[-1])
    is_low = lax.broadcasted_iota(jnp.int32, high.shape, 3) == 1
    page_bounds = jnp.where(is_low, 0 - high, high)
    paged_cache = pages.reshape(layer_count, page_dev, *kv_cache.shape[2:])
    return paged_cache, page_bounds


def solution(mesh):
    in_specs = (
        P(None, ("groups", "seq"), "head", "rep", None),
        P("groups", None),
        P("groups", None),
    )
    out_specs = (
        P(None, ("groups", "seq"), "head", "rep", None),
        P(None, ("groups", "seq"), "head", None, None),
    )
    return jax.shard_map(
        on_device, mesh=mesh, in_specs=in_specs, out_specs=out_specs, check_vma=False
    )
```

```python
import functools

import jax
import jax.numpy as jnp
from jax import lax
from jax.experimental import pallas as pl
from jax.experimental.pallas import tpu as pltpu
from jax.sharding import PartitionSpec as P


def forward(fetches, leaves):
    for arrive, leave in zip(fetches, leaves):
        arrive.wait()
        leave.start()
    for leave in leaves:
        leave.wait()


def pack_kernel(index_ref, cache_ref, out_ref, stage, sem_in, sem_out):
    layers = index_ref.shape[0]
    owners = out_ref.shape[0] // layers
    offset = index_ref.shape[1] - owners
    keys = [(layer, owner) for owner in range(owners) for layer in range(layers)]
    fetches = [
        pltpu.make_async_copy(
            cache_ref.at[layer, index_ref[layer, offset + owner], 0], stage.at[k], sem_in.at[k]
        )
        for k, (layer, owner) in enumerate(keys)
    ]
    leaves = [
        pltpu.make_async_copy(stage.at[k], out_ref.at[k], sem_out.at[k]) for k in range(len(keys))
    ]
    for copy in fetches:
        copy.start()
    forward(fetches, leaves)


def pack_seconds(index, cache, count):
    block = cache.shape[3:]
    return pl.pallas_call(
        pack_kernel,
        grid_spec=pltpu.PrefetchScalarGridSpec(
            num_scalar_prefetch=1,
            grid=(1,),
            in_specs=[pl.BlockSpec(memory_space=pltpu.HBM)],
            out_specs=pl.BlockSpec(memory_space=pltpu.HBM),
            scratch_shapes=[
                pltpu.VMEM((count, *block), cache.dtype),
                pltpu.SemaphoreType.DMA((count,)),
                pltpu.SemaphoreType.DMA((count,)),
            ],
        ),
        out_shape=jax.ShapeDtypeStruct((count, *block), cache.dtype),
        compiler_params=pltpu.CompilerParams(vmem_limit_bytes=8 << 20),
    )(index, cache)


def plan_kernel(
    owners, blk_dev, page_dev,
    keep_hbm, slot_hbm, cache_ref,
    payload_ref, left_ref, right_ref, table_ref, branch_ref, many_ref,
    keep_ref, slot_ref, shard, lists, held_lists, sem_in, sem_shard, sem_out, sem_list,
):
    inputs = [
        pltpu.make_async_copy(keep_hbm, keep_ref, sem_in.at[0]),
        pltpu.make_async_copy(slot_hbm, slot_ref, sem_in.at[1]),
    ]
    for copy in inputs:
        copy.start()
    parts = sem_shard.shape[1]
    size = blk_dev // parts
    shards = []
    for layer in range(cache_ref.shape[0]):
        for part in range(parts):
            which = (layer, pl.ds(part * size, size))
            shards.append(
                pltpu.make_async_copy(
                    cache_ref.at[which], shard.at[which], sem_shard.at[layer, part]
                )
            )
    for copy in shards:
        copy.start()
    layers, entries = keep_ref.shape
    slots, none = owners * layers, 2 * owners * layers
    late = 8 * slots
    me = lax.axis_index("seq")
    block_bits, page_bits = blk_dev.bit_length() - 1, page_dev.bit_length() - 1

    row = lax.broadcasted_iota(jnp.int32, (owners, entries), 0)
    square_row = lax.broadcasted_iota(jnp.int32, (owners, owners), 0)
    square_lane = lax.broadcasted_iota(jnp.int32, (owners, owners), 1)
    lane = lax.broadcasted_iota(jnp.int32, (owners, lists.shape[1]), 1)

    def most(values):
        return jnp.max(values.astype(jnp.float32), axis=1, keepdims=True).astype(jnp.int32)

    for copy in inputs:
        copy.wait()
    tables = jnp.zeros(lists.shape, jnp.int32)
    for layer in range(layers):
        keep, slot = keep_ref[pl.ds(layer, 1), :], slot_ref[pl.ds(layer, 1), :]
        source, owner = keep >> block_bits, slot >> page_bits
        chosen = (owner == row) & (source == me)
        local = keep - me * blk_dev
        first = blk_dev - 1 - most(jnp.where(chosen, blk_dev - 1 - local, 0))
        second = most(jnp.where(chosen, local, 0))
        gap = owner - source
        gap = jnp.where(gap < 0, gap + owners, gap)
        by_gap = jnp.where((gap == row) & (keep >= 0), 1.0, 0.0).astype(jnp.bfloat16)
        by_source = jnp.where(source == row, 1.0, 0.0).astype(jnp.bfloat16)
        count = lax.dot_general(
            by_gap, by_source, (((1,), (1,)), ((), ())), preferred_element_type=jnp.float32
        )
        active = (jnp.max(count, axis=1, keepdims=True) > 1.5).astype(jnp.int32)
        held = most(jnp.where(slot == me * page_dev + row, keep, -1))
        across = jnp.max(
            jnp.where(square_row == square_lane, held, -1).astype(jnp.float32), axis=0, keepdims=True
        ).astype(jnp.int32)
        origin = held >> block_bits
        again = most(jnp.where((across >> block_bits == origin) & (across < held), 1, 0))
        found = jnp.where(held < 0, -1, origin * layers + layer + again * late)
        for kind, values in enumerate((first, second, active, found)):
            tables = jnp.where(lane == kind * layers + layer, values, tables)
    lists[...] = tables
    copy = pltpu.make_async_copy(lists, held_lists, sem_list)
    copy.start()
    copy.wait()

    def listed(kind, layer, index):
        return held_lists[index, kind * layers + layer]

    for copy in shards:
        copy.wait()
    for owner in range(owners):
        for layer in range(layers):
            block = shard.at[layer, listed(0, layer, owner), 0]
            target = payload_ref.at[owner * layers + layer]
            pltpu.make_async_copy(block, target, sem_out.at[0]).start()

    class_a, class_b, total = jnp.int32(none), jnp.int32(none), jnp.int32(0)
    for layer in range(layers):
        for gap in range(owners):
            on = listed(2, layer, gap)
            class_b = jnp.where((on > 0) & (total == 1), layer * owners + gap, class_b)
            class_a = jnp.where((on > 0) & (total == 0), layer * owners + gap, class_a)
            total = total + on
    many = (total > 2).astype(jnp.int32)
    shift_a = jnp.where(class_a < none, lax.rem(class_a, owners), 0)
    shift_b = jnp.where(class_b < none, lax.rem(class_b, owners), 0)
    flip = shift_a > shift_b
    class_a, class_b = jnp.where(flip, class_b, class_a), jnp.where(flip, class_a, class_b)
    shift_a, shift_b = jnp.where(flip, shift_b, shift_a), jnp.where(flip, shift_a, shift_b)
    extras = []
    for number, by, target in ((class_a, shift_a, left_ref), (class_b, shift_b, right_ref)):
        layer = jnp.where(number < none, lax.div(number, owners), 0)
        index = listed(1, layer, lax.rem(me + by, owners))
        sem = sem_out.at[1 + len(extras)]
        extras.append(pltpu.make_async_copy(shard.at[layer, index, 0], target, sem))
        extras[-1].start()
    branch_ref[0] = lax.div(shift_b * (shift_b + 1), 2) + shift_a
    many_ref[0] = many

    for layer in range(layers):
        for index in range(owners):
            table_ref[layer, page_dev + index] = listed(1, layer, index)
            slot = listed(3, layer, index)
            plain = jnp.where(slot >= late, slot - late, slot)
            back = lax.rem(me - lax.div(plain, layers) + owners, owners)
            moved = jnp.where(layer * owners + back == class_a, slots, slots + 1)
            moved = jnp.where(many > 0, slots + 3 + plain, moved)
            moved = jnp.where(slot >= late, moved, slot)
            table_ref[layer, index] = jnp.where(slot < 0, slots + 2, moved)

    pltpu.make_async_copy(payload_ref, payload_ref, sem_out.at[0]).wait()
    for copy in extras:
        copy.wait()


def plan_and_pack(keep_list, page_slot, cache, owners):
    layers, entries = keep_list.shape
    slots, block = owners * layers, cache.shape[3:]
    page_dev = entries // owners
    smem = pl.BlockSpec(memory_space=pltpu.SMEM)
    hbm = pl.BlockSpec(memory_space=pltpu.HBM)
    one = jax.ShapeDtypeStruct(block, cache.dtype)
    return pl.pallas_call(
        functools.partial(plan_kernel, owners, cache.shape[1], page_dev),
        in_specs=[hbm, hbm, hbm],
        out_specs=[hbm, hbm, hbm, smem, smem, smem],
        scratch_shapes=[
            pltpu.VMEM(keep_list.shape, jnp.int32),
            pltpu.VMEM(page_slot.shape, jnp.int32),
            pltpu.VMEM(cache.shape, cache.dtype),
            pltpu.VMEM((owners, 128), jnp.int32),
            pltpu.SMEM((owners, 128), jnp.int32),
            pltpu.SemaphoreType.DMA((2,)),
            pltpu.SemaphoreType.DMA((layers, 4)),
            pltpu.SemaphoreType.DMA((3,)),
            pltpu.SemaphoreType.DMA,
        ],
        out_shape=[
            jax.ShapeDtypeStruct((slots, *block), cache.dtype),
            one,
            one,
            jax.ShapeDtypeStruct((layers, page_dev + owners), jnp.int32),
            jax.ShapeDtypeStruct((1,), jnp.int32),
            jax.ShapeDtypeStruct((1,), jnp.int32),
        ],
        compiler_params=pltpu.CompilerParams(vmem_limit_bytes=60 << 20),
    )(keep_list, page_slot, cache)


def place_kernel(
    table_ref, many_ref, base_ref, left_ref, right_ref, extra_ref,
    out_ref, bounds_ref, spare, high, low, rows, sem, spare_sem,
):
    slots, head_width = base_ref.shape[0], base_ref.shape[-1] // 2
    pages = out_ref.shape[0]
    page_dev = pages // table_ref.shape[0]
    spare[0] = left_ref[...]
    spare[1] = right_ref[...]
    spare[2] = jnp.zeros_like(left_ref)

    def entry(i):
        return table_ref[i // page_dev, i % page_dev]

    for i in range(pages):
        t = entry(i)

        @pl.when(t < slots)
        def _():
            block = base_ref.at[jnp.minimum(t, slots - 1)]
            pltpu.make_async_copy(block, out_ref.at[i], sem).start()

    def extremes(k, ref):
        keys = ref[:, :head_width]
        high[pl.ds(k, 1), :] = jnp.max(keys, axis=0, keepdims=True).astype(jnp.float32)
        low[pl.ds(k, 1), :] = -jnp.min(keys, axis=0, keepdims=True).astype(jnp.float32)

    for k in range(slots):
        extremes(k, base_ref.at[k])
    for k in range(3):
        extremes(slots + k, spare.at[k])

    @pl.when(many_ref[0] != 0)
    def _():
        copy = pltpu.make_async_copy(extra_ref, spare.at[pl.ds(3, slots)], spare_sem)
        copy.start()
        copy.wait()

        @pl.loop(0, slots)
        def _(k):
            extremes(slots + 3 + k, spare.at[3 + k])

    for i in range(pages):
        t = entry(i)

        @pl.when(t >= slots)
        def _():
            block = spare.at[jnp.maximum(t - slots, 0)]
            pltpu.make_async_copy(block, out_ref.at[i], sem).start()

        rows[pl.ds(2 * i, 1), :] = high[pl.ds(t, 1), :]
        rows[pl.ds(2 * i + 1, 1), :] = low[pl.ds(t, 1), :]

    bounds_ref[...] = rows[...].astype(bounds_ref.dtype)
    pltpu.make_async_copy(out_ref, out_ref, sem).wait()


def place_pages(table, many, base, left, right, extra, pages):
    block, head_width = base.shape[1:], base.shape[-1] // 2
    vmem = pl.BlockSpec(memory_space=pltpu.VMEM)
    hbm = pl.BlockSpec(memory_space=pltpu.HBM)
    return pl.pallas_call(
        place_kernel,
        grid_spec=pltpu.PrefetchScalarGridSpec(
            num_scalar_prefetch=2,
            grid=(1,),
            in_specs=[vmem, vmem, vmem, hbm],
            out_specs=[hbm, vmem],
            scratch_shapes=[
                pltpu.VMEM((3 + base.shape[0], *block), base.dtype),
                pltpu.VMEM((3 + 2 * base.shape[0], head_width), jnp.float32),
                pltpu.VMEM((3 + 2 * base.shape[0], head_width), jnp.float32),
                pltpu.VMEM((2 * pages, head_width), jnp.float32),
                pltpu.SemaphoreType.DMA,
                pltpu.SemaphoreType.DMA,
            ],
        ),
        out_shape=[
            jax.ShapeDtypeStruct((pages, *block), base.dtype),
            jax.ShapeDtypeStruct((2 * pages, head_width), base.dtype),
        ],
        compiler_params=pltpu.CompilerParams(vmem_limit_bytes=8 << 20),
    )(table, many, base, left, right, extra)


def swap(block, shift, size):
    if shift == 0:
        return block
    return lax.ppermute(block, "seq", [(s, (s + shift) % size) for s in range(size)])


def on_device(kv_cache, keep_list, page_slot):
    layer_count, page_count = keep_list.shape
    seq_count = lax.axis_size("seq")
    page_dev = page_count // seq_count
    slots = seq_count * layer_count

    def exchange(blocks):
        shaped = blocks.reshape(seq_count, layer_count, *blocks.shape[1:])
        moved = lax.all_to_all(shaped, "seq", split_axis=0, concat_axis=0, tiled=True)
        return moved.reshape(blocks.shape)

    payload, one, two, table, branch, many = plan_and_pack(
        keep_list, page_slot, kv_cache, seq_count
    )
    branch, many = branch.reshape(()), many.reshape(())
    base = exchange(payload)

    branches = [
        lambda one, two, one_by=a, two_by=b: (
            swap(one, one_by, seq_count),
            swap(two, two_by, seq_count),
        )
        for b in range(seq_count)
        for a in range(b + 1)
    ]
    left, right = lax.switch(branch, branches, one, two)

    def all_seconds(state):
        rounds, index, _ = lax.optimization_barrier(state)
        return rounds - 1, index, exchange(pack_seconds(index, kv_cache, slots))

    base, payload, many = lax.optimization_barrier((base, payload, many))
    _, table, extra = lax.while_loop(lambda state: state[0] > 0, all_seconds, (many, table, payload))

    pages, half = place_pages(
        table, many.reshape(1), base, left, right, extra, layer_count * page_dev
    )
    halves = lax.all_gather(half, "rep")
    high = jnp.max(halves, axis=0).reshape(layer_count, page_dev, 1, 2, half.shape[-1])
    is_low = lax.broadcasted_iota(jnp.int32, high.shape, 3) == 1
    page_bounds = jnp.where(is_low, 0 - high, high)
    paged_cache = pages.reshape(layer_count, page_dev, *kv_cache.shape[2:])
    return paged_cache, page_bounds


def solution(mesh):
    in_specs = (
        P(None, ("groups", "seq"), "head", "rep", None),
        P("groups", None),
        P("groups", None),
    )
    out_specs = (
        P(None, ("groups", "seq"), "head", "rep", None),
        P(None, ("groups", "seq"), "head", None, None),
    )
    return jax.shard_map(
        on_device, mesh=mesh, in_specs=in_specs, out_specs=out_specs, check_vma=False
    )
```

```python
import functools

import jax
import jax.numpy as jnp
from jax import lax
from jax.experimental import pallas as pl
from jax.experimental.pallas import tpu as pltpu
from jax.sharding import PartitionSpec as P


def forward(fetches, leaves):
    for arrive, leave in zip(fetches, leaves):
        arrive.wait()
        leave.start()
    for leave in leaves:
        leave.wait()


def pack_kernel(index_ref, cache_ref, out_ref, stage, sem_in, sem_out):
    layers = index_ref.shape[0]
    owners = out_ref.shape[0] // layers
    offset = index_ref.shape[1] - owners
    keys = [(layer, owner) for owner in range(owners) for layer in range(layers)]
    fetches = [
        pltpu.make_async_copy(
            cache_ref.at[layer, index_ref[layer, offset + owner], 0], stage.at[k], sem_in.at[k]
        )
        for k, (layer, owner) in enumerate(keys)
    ]
    leaves = [
        pltpu.make_async_copy(stage.at[k], out_ref.at[k], sem_out.at[k]) for k in range(len(keys))
    ]
    for copy in fetches:
        copy.start()
    forward(fetches, leaves)


def pack_seconds(index, cache, count):
    block = cache.shape[3:]
    return pl.pallas_call(
        pack_kernel,
        grid_spec=pltpu.PrefetchScalarGridSpec(
            num_scalar_prefetch=1,
            grid=(1,),
            in_specs=[pl.BlockSpec(memory_space=pltpu.HBM)],
            out_specs=pl.BlockSpec(memory_space=pltpu.HBM),
            scratch_shapes=[
                pltpu.VMEM((count, *block), cache.dtype),
                pltpu.SemaphoreType.DMA((count,)),
                pltpu.SemaphoreType.DMA((count,)),
            ],
        ),
        out_shape=jax.ShapeDtypeStruct((count, *block), cache.dtype),
        compiler_params=pltpu.CompilerParams(vmem_limit_bytes=8 << 20),
    )(index, cache)


def plan_kernel(
    owners, blk_dev, page_dev,
    keep_hbm, slot_hbm, cache_ref,
    payload_ref, left_ref, right_ref, table_ref, branch_ref, many_ref,
    keep_ref, slot_ref, shard, lists, held_lists, sem_in, sem_shard, sem_out, sem_list,
):
    inputs = [
        pltpu.make_async_copy(keep_hbm, keep_ref, sem_in.at[0]),
        pltpu.make_async_copy(slot_hbm, slot_ref, sem_in.at[1]),
    ]
    for copy in inputs:
        copy.start()
    parts = sem_shard.shape[1]
    size = blk_dev // parts
    shards = []
    for layer in range(cache_ref.shape[0]):
        for part in range(parts):
            which = (layer, pl.ds(part * size, size))
            shards.append(
                pltpu.make_async_copy(
                    cache_ref.at[which], shard.at[which], sem_shard.at[layer, part]
                )
            )
    for copy in shards:
        copy.start()
    layers, entries = keep_ref.shape
    slots, none = owners * layers, 2 * owners * layers
    late = 8 * slots
    me = lax.axis_index("seq")
    block_bits, page_bits = blk_dev.bit_length() - 1, page_dev.bit_length() - 1

    row = lax.broadcasted_iota(jnp.int32, (owners, entries), 0)
    square_row = lax.broadcasted_iota(jnp.int32, (owners, owners), 0)
    square_lane = lax.broadcasted_iota(jnp.int32, (owners, owners), 1)
    lane = lax.broadcasted_iota(jnp.int32, (owners, lists.shape[1]), 1)

    def most(values):
        return jnp.max(values.astype(jnp.float32), axis=1, keepdims=True).astype(jnp.int32)

    for copy in inputs:
        copy.wait()
    tables = jnp.zeros(lists.shape, jnp.int32)
    for layer in range(layers):
        keep, slot = keep_ref[pl.ds(layer, 1), :], slot_ref[pl.ds(layer, 1), :]
        source, owner = keep >> block_bits, slot >> page_bits
        chosen = (owner == row) & (source == me)
        local = keep - me * blk_dev
        first = blk_dev - 1 - most(jnp.where(chosen, blk_dev - 1 - local, 0))
        second = most(jnp.where(chosen, local, 0))
        gap = owner - source
        gap = jnp.where(gap < 0, gap + owners, gap)
        by_gap = jnp.where((gap == row) & (keep >= 0), 1.0, 0.0).astype(jnp.bfloat16)
        by_source = jnp.where(source == row, 1.0, 0.0).astype(jnp.bfloat16)
        count = lax.dot_general(
            by_gap, by_source, (((1,), (1,)), ((), ())), preferred_element_type=jnp.float32
        )
        active = (jnp.max(count, axis=1, keepdims=True) > 1.5).astype(jnp.int32)
        held = most(jnp.where(slot == me * page_dev + row, keep, -1))
        across = jnp.max(
            jnp.where(square_row == square_lane, held, -1).astype(jnp.float32), axis=0, keepdims=True
        ).astype(jnp.int32)
        origin = held >> block_bits
        again = most(jnp.where((across >> block_bits == origin) & (across < held), 1, 0))
        found = jnp.where(held < 0, -1, origin * layers + layer + again * late)
        for kind, values in enumerate((first, second, active, found)):
            tables = jnp.where(lane == kind * layers + layer, values, tables)
    lists[...] = tables
    copy = pltpu.make_async_copy(lists, held_lists, sem_list)
    copy.start()
    copy.wait()

    def listed(kind, layer, index):
        return held_lists[index, kind * layers + layer]

    for copy in shards:
        copy.wait()
    for owner in range(owners):
        for layer in range(layers):
            block = shard.at[layer, listed(0, layer, owner), 0]
            target = payload_ref.at[owner * layers + layer]
            pltpu.make_async_copy(block, target, sem_out.at[0]).start()

    class_a, class_b, total = jnp.int32(none), jnp.int32(none), jnp.int32(0)
    for layer in range(layers):
        for gap in range(owners):
            on = listed(2, layer, gap)
            class_b = jnp.where((on > 0) & (total == 1), layer * owners + gap, class_b)
            class_a = jnp.where((on > 0) & (total == 0), layer * owners + gap, class_a)
            total = total + on
    many = (total > 2).astype(jnp.int32)
    shift_a = jnp.where(class_a < none, lax.rem(class_a, owners), 0)
    shift_b = jnp.where(class_b < none, lax.rem(class_b, owners), 0)
    flip = shift_a > shift_b
    class_a, class_b = jnp.where(flip, class_b, class_a), jnp.where(flip, class_a, class_b)
    shift_a, shift_b = jnp.where(flip, shift_b, shift_a), jnp.where(flip, shift_a, shift_b)
    extras = []
    for number, by, target in ((class_a, shift_a, left_ref), (class_b, shift_b, right_ref)):
        layer = jnp.where(number < none, lax.div(number, owners), 0)
        index = listed(1, layer, lax.rem(me + by, owners))
        sem = sem_out.at[1 + len(extras)]
        extras.append(pltpu.make_async_copy(shard.at[layer, index, 0], target, sem))
        extras[-1].start()
    branch_ref[0] = lax.div(shift_b * (shift_b + 1), 2) + shift_a
    many_ref[0] = many

    for layer in range(layers):
        for index in range(owners):
            table_ref[layer, page_dev + index] = listed(1, layer, index)
            slot = listed(3, layer, index)
            plain = jnp.where(slot >= late, slot - late, slot)
            back = lax.rem(me - lax.div(plain, layers) + owners, owners)
            moved = jnp.where(layer * owners + back == class_a, slots, slots + 1)
            moved = jnp.where(many > 0, slots + 3 + plain, moved)
            moved = jnp.where(slot >= late, moved, slot)
            table_ref[layer, index] = jnp.where(slot < 0, slots + 2, moved)

    pltpu.make_async_copy(payload_ref, payload_ref, sem_out.at[0]).wait()
    for copy in extras:
        copy.wait()


def plan_and_pack(keep_list, page_slot, cache, owners):
    layers, entries = keep_list.shape
    slots, block = owners * layers, cache.shape[3:]
    page_dev = entries // owners
    smem = pl.BlockSpec(memory_space=pltpu.SMEM)
    hbm = pl.BlockSpec(memory_space=pltpu.HBM)
    one = jax.ShapeDtypeStruct(block, cache.dtype)
    return pl.pallas_call(
        functools.partial(plan_kernel, owners, cache.shape[1], page_dev),
        in_specs=[hbm, hbm, hbm],
        out_specs=[hbm, hbm, hbm, smem, smem, smem],
        scratch_shapes=[
            pltpu.VMEM(keep_list.shape, jnp.int32),
            pltpu.VMEM(page_slot.shape, jnp.int32),
            pltpu.VMEM(cache.shape, cache.dtype),
            pltpu.VMEM((owners, 128), jnp.int32),
            pltpu.SMEM((owners, 128), jnp.int32),
            pltpu.SemaphoreType.DMA((2,)),
            pltpu.SemaphoreType.DMA((layers, 4)),
            pltpu.SemaphoreType.DMA((3,)),
            pltpu.SemaphoreType.DMA,
        ],
        out_shape=[
            jax.ShapeDtypeStruct((slots, *block), cache.dtype),
            one,
            one,
            jax.ShapeDtypeStruct((layers, page_dev + owners), jnp.int32),
            jax.ShapeDtypeStruct((1,), jnp.int32),
            jax.ShapeDtypeStruct((1,), jnp.int32),
        ],
        compiler_params=pltpu.CompilerParams(vmem_limit_bytes=60 << 20),
    )(keep_list, page_slot, cache)


def place_kernel(
    table_ref, many_ref, base_ref, left_ref, right_ref, extra_ref,
    out_ref, bounds_ref, spare, rows, sem, spare_sem,
):
    slots, head_width = base_ref.shape[0], base_ref.shape[-1] // 2
    pages = out_ref.shape[0]
    page_dev = pages // table_ref.shape[0]
    spare[0] = left_ref[...]
    spare[1] = right_ref[...]
    spare[2] = jnp.zeros_like(left_ref)

    def entry(i):
        return table_ref[i // page_dev, i % page_dev]

    for i in range(pages):
        t = entry(i)

        @pl.when(t < slots)
        def _():
            block = base_ref.at[jnp.minimum(t, slots - 1)]
            pltpu.make_async_copy(block, out_ref.at[i], sem).start()

    @pl.when(many_ref[0] != 0)
    def _():
        copy = pltpu.make_async_copy(extra_ref, spare.at[pl.ds(3, slots)], spare_sem)
        copy.start()
        copy.wait()

    for i in range(pages):
        t = entry(i)
        plain = base_ref[jnp.minimum(t, slots - 1), :, :head_width]
        other = spare[jnp.maximum(t - slots, 0), :, :head_width]
        keys = jnp.where(t < slots, plain, other)
        rows[2 * i : 2 * i + 1, :] = jnp.max(keys, axis=0, keepdims=True).astype(jnp.float32)
        rows[2 * i + 1 : 2 * i + 2, :] = -jnp.min(keys, axis=0, keepdims=True).astype(jnp.float32)

    for i in range(pages):
        t = entry(i)

        @pl.when(t >= slots)
        def _():
            block = spare.at[jnp.maximum(t - slots, 0)]
            pltpu.make_async_copy(block, out_ref.at[i], sem).start()

    bounds_ref[...] = rows[...].astype(bounds_ref.dtype)
    pltpu.make_async_copy(out_ref, out_ref, sem).wait()


def place_pages(table, many, base, left, right, extra, pages):
    block, head_width = base.shape[1:], base.shape[-1] // 2
    vmem = pl.BlockSpec(memory_space=pltpu.VMEM)
    hbm = pl.BlockSpec(memory_space=pltpu.HBM)
    return pl.pallas_call(
        place_kernel,
        grid_spec=pltpu.PrefetchScalarGridSpec(
            num_scalar_prefetch=2,
            grid=(1,),
            in_specs=[vmem, vmem, vmem, hbm],
            out_specs=[hbm, vmem],
            scratch_shapes=[
                pltpu.VMEM((3 + base.shape[0], *block), base.dtype),
                pltpu.VMEM((2 * pages, head_width), jnp.float32),
                pltpu.SemaphoreType.DMA,
                pltpu.SemaphoreType.DMA,
            ],
        ),
        out_shape=[
            jax.ShapeDtypeStruct((pages, *block), base.dtype),
            jax.ShapeDtypeStruct((2 * pages, head_width), base.dtype),
        ],
        compiler_params=pltpu.CompilerParams(vmem_limit_bytes=8 << 20),
    )(table, many, base, left, right, extra)


def swap(block, shift, size):
    if shift == 0:
        return block
    return lax.ppermute(block, "seq", [(s, (s + shift) % size) for s in range(size)])


def on_device(kv_cache, keep_list, page_slot):
    layer_count, page_count = keep_list.shape
    seq_count = lax.axis_size("seq")
    page_dev = page_count // seq_count
    slots = seq_count * layer_count

    def exchange(blocks):
        shaped = blocks.reshape(seq_count, layer_count, *blocks.shape[1:])
        moved = lax.all_to_all(shaped, "seq", split_axis=0, concat_axis=0, tiled=True)
        return moved.reshape(blocks.shape)

    payload, one, two, table, branch, many = plan_and_pack(
        keep_list, page_slot, kv_cache, seq_count
    )
    branch, many = branch.reshape(()), many.reshape(())
    base = exchange(payload)

    branches = [
        lambda one, two, one_by=a, two_by=b: (
            swap(one, one_by, seq_count),
            swap(two, two_by, seq_count),
        )
        for b in range(seq_count)
        for a in range(b + 1)
    ]
    left, right = lax.switch(branch, branches, one, two)

    def all_seconds(state):
        rounds, index, _ = lax.optimization_barrier(state)
        return rounds - 1, index, exchange(pack_seconds(index, kv_cache, slots))

    base, payload = lax.optimization_barrier((base, payload))
    _, table, extra = lax.while_loop(lambda state: state[0] > 0, all_seconds, (many, table, payload))

    pages, half = place_pages(
        table, many.reshape(1), base, left, right, extra, layer_count * page_dev
    )
    halves = lax.all_gather(half, "rep")
    high = jnp.max(halves, axis=0).reshape(layer_count, page_dev, 1, 2, half.shape[-1])
    is_low = lax.broadcasted_iota(jnp.int32, high.shape, 3) == 1
    page_bounds = jnp.where(is_low, 0 - high, high)
    paged_cache = pages.reshape(layer_count, page_dev, *kv_cache.shape[2:])
    return paged_cache, page_bounds


def solution(mesh):
    in_specs = (
        P(None, ("groups", "seq"), "head", "rep", None),
        P("groups", None),
        P("groups", None),
    )
    out_specs = (
        P(None, ("groups", "seq"), "head", "rep", None),
        P(None, ("groups", "seq"), "head", None, None),
    )
    return jax.shard_map(
        on_device, mesh=mesh, in_specs=in_specs, out_specs=out_specs, check_vma=False
    )
```
